32 devices in a mesh: row: 8 (over z, core), col: 4 (over y, x).
Axes of the slice: x: 2, y: 2, z: 4, core: 2. Of those that a mesh axis runs over, the one named last changes fastest.
Arguments:
- loadings: bfloat16 [8, 32768, 1024], P(None, 'row', 'col'), may hold values from -6 to 6
- weights: bfloat16 [8, 32768, 512], P(None, 'row', 'col'), may hold values from -0.03125 to 0.03125
- specific: float32 [8, 32768], P(None, 'row'), may hold values from 0.2 to 5
- factor_cov: float32 [8, 1024, 1024], P(None, 'col'), may hold values from -0.001953125 to 0.0048828125, as said below
Outputs:
- portfolio_cov: float32 [8, 512, 512], P(None, 'row', 'col')
The draws below stay inside these ranges and needn't reach their ends.
Inputs may be any that keep to these rules, and one draw needn't show every extreme that they name: `factor_cov`: each day's matrix is a symmetric positive definite factor covariance of order 1024.
All inputs are finite; a program needn't handle non-finite values.
Results may differ from the reference program's by a relative error of at most 0.0003.
Values may be sent and summed in bfloat16 or wider, within the bound.
A program may use at most 128 MiB of HBM per device.

```python
import math
import jax
import jax.numpy as jnp
from jax import lax

N = 32768
R = 1024
K = 512
DAYS = 8


def draw_factor_cov(key, part):
    first_key, second_key = jax.random.split(jax.random.fold_in(key, 11))
    noise = jax.random.normal(first_key, (DAYS, R, R), jnp.float32)
    symmetric = (noise + jnp.swapaxes(noise, 1, 2)) / jnp.sqrt(2.0 * R)
    variances = jax.random.uniform(second_key, (DAYS, R), jnp.float32, 1.0, 3.0)
    identity = jnp.eye(R, dtype=jnp.float32)
    return (identity[None, :, :] * variances[:, :, None] + 0.4 * symmetric) / R


def steps_of(rng, extent, pieces, smallest, largest):
    loudness, own = 1.0, jax.random.fold_in(rng, 6)
    for position, parts in pieces:
        steps = jnp.exp(jax.random.uniform(jax.random.fold_in(own, position), (parts,), jnp.float32, smallest / len(pieces), largest / len(pieces)))
        loudness = loudness * jnp.repeat(steps, extent[position] // parts).reshape([-1 if axis == position else 1 for axis in range(len(extent))])
    return loudness


def normal_values(rng, dims, spread, reach, cuts=(), kind=jnp.bfloat16):
    result = spread * jax.random.normal(rng, dims, jnp.float32)
    if cuts:
        result = result * steps_of(rng, dims, cuts, -0.22, 0.18)
    return jnp.clip(result, -reach, reach).astype(kind)


def setup_inputs(seed: int = 0) -> dict:
    keys = jax.random.split(jax.random.key(seed), 5)
    return {
        "loadings": normal_values(keys[0], (DAYS, N, R), 1.0, 6.0, ((1, 8), (2, 4))),
        "weights": normal_values(keys[1], (DAYS, N, K), N ** -0.5, 0.03125, ((1, 8), (2, 4))),
        "specific": jnp.clip(jnp.exp(math.log(5.0) - 3.218876 * jax.random.uniform(keys[2], (DAYS, N), jnp.float32) ** steps_of(keys[2], (DAYS, N), ((1, 8),), -0.2, 0.2)), 0.2, 5.0),
        "factor_cov": draw_factor_cov(jax.random.fold_in(keys[4], 71), 0),
    }


def one_day(operands):
    loadings, weights, specific, factor_cov = operands
    exposure = jnp.dot(loadings.T, weights, preferred_element_type=jnp.float32)
    weighted = (specific[:, None] * weights.astype(jnp.float32)).astype(jnp.bfloat16)
    specific_cov = jnp.dot(weights.T, weighted, preferred_element_type=jnp.float32)
    left = jnp.dot(exposure.T, factor_cov, precision=lax.Precision.HIGHEST)
    return jnp.dot(left, exposure, precision=lax.Precision.HIGHEST) + specific_cov


def reference(loadings, weights, specific, factor_cov):
    return lax.map(one_day, (loadings, weights, specific, factor_cov))
```

```python
import functools

import jax
import jax.numpy as jnp
from jax import lax
from jax.experimental import pallas as pl
from jax.experimental.pallas import tpu as pltpu
from jax.sharding import PartitionSpec as P

F32, BF16 = jnp.float32, jnp.bfloat16
HIGHEST = lax.Precision.HIGHEST


def by_dim(a, b, dim, precision=None):
    return lax.dot_general(
        a, b, (((dim,), (dim,)), ((), ())), precision=precision, preferred_element_type=F32
    )


def kernel(
    rows, cols, load_hbm, weight_hbm, spec_ref, fcov_hbm, out_ref,
    held, load, fcov, weighted, part, part_in, exp_rows, exp_cols, own_spec, prod, prod_in,
    w_sem, l_sem, f_sem, g_send, g_recv, p_send, p_recv,
    er_send, er_recv, ec_send, ec_recv, q_send, q_recv,
):
    days, assets, factors = load_hbm.shape
    ports = weight_hbm.shape[2]
    slab = ports * cols // rows
    half = assets // 2
    row, col = lax.axis_index("row"), lax.axis_index("col")
    near_x = col + 1 - 2 * (col % 2)
    near_y = (col + 2) % 4
    far = 3 - col

    def to_row(r):
        return {"row": r, "col": col}

    def to_col(c):
        return {"row": row, "col": c}

    def remote(src, dst, send, recv, where):
        return pltpu.make_async_remote_copy(
            src_ref=src, dst_ref=dst, send_sem=send, recv_sem=recv,
            device_id=where, device_id_type=pl.DeviceIdType.MESH,
        )

    def gather(d, lane, block):
        ref = held.at[d, block]
        if lane == 2:
            ref = held.at[d, block, pl.ds(0, half)]
        if lane == 3:
            ref = held.at[d, block, pl.ds(half, half)]
        where = near_x if lane in (0, 3) else near_y
        return remote(ref, ref, g_send.at[d, lane], g_recv.at[d, lane], to_col(where))

    def own_weights(d):
        return pltpu.make_async_copy(weight_hbm.at[d], held.at[d, col], w_sem.at[d])

    def get_load(d):
        return pltpu.make_async_copy(load_hbm.at[d], load.at[d % 2], l_sem.at[d % 2])

    def get_fcov(d):
        return pltpu.make_async_copy(fcov_hbm.at[d], fcov.at[d % 2], f_sem.at[d % 2])

    def part_copy(d, other, landed):
        return remote(
            part.at[d % 2, pl.ds(pl.multiple_of(other * slab, slab), slab)],
            part_in.at[d, landed], p_send.at[d, other], p_recv.at[d, landed], to_row(other),
        )

    def exp_row_copy(d, other, landed):
        ref = exp_rows.at[d, pl.ds(pl.multiple_of(landed * slab, slab), slab)]
        return remote(ref, ref, er_send.at[d, other], er_recv.at[d, landed], to_row(other))

    def exp_col_copy(d, other, landed):
        ref = exp_cols.at[d, landed]
        return remote(ref, ref, ec_send.at[d, other], ec_recv.at[d, landed], to_col(other))

    def prod_copy(d, other, landed):
        return remote(
            prod.at[d, other], prod_in.at[d, landed],
            q_send.at[d, other], q_recv.at[d, landed], to_col(other),
        )

    def row_peers():
        return [(row + step) % rows for step in range(1, rows)]

    def col_peers():
        return [near_x, near_y, far]

    def send_own(d):
        own_weights(d).wait()
        gather(d, 0, col).start()
        gather(d, 1, col).start()

    def pass_on(d):
        gather(d, 0, near_x).wait_recv()
        gather(d, 2, near_x).start()
        gather(d, 1, near_y).wait_recv()
        gather(d, 3, near_y).start()

    def partial_sums(d):
        slot = d % 2
        scales = spec_ref[d]
        groups = scales.shape[0]
        copies = -(-128 // groups)
        tall = jnp.concatenate([scales] * copies, axis=0).T
        for i in range(groups):
            span = pl.ds(i * 128, 128)
            block = held[d, col, span].astype(F32) * tall[:, i : i + 1]
            weighted[span] = block.astype(BF16)

        @pl.when(d >= 2)
        def _():
            for peer in row_peers():
                part_copy(d - 2, peer, row).wait_send()

        gather(d, 2, far).wait_recv()
        gather(d, 3, far).wait_recv()
        get_load(d).wait()

        def block(j, carry):
            lhs = held[d, j]
            span = pl.ds(pl.multiple_of(j * ports, ports), ports)
            part[slot, span, pl.ds(0, factors)] = by_dim(lhs, load[slot], 0)
            part[slot, span, pl.ds(factors, ports)] = by_dim(lhs, weighted[...], 0)
            return carry

        lax.fori_loop(0, cols, block, 0)
        for peer in row_peers():
            part_copy(d, peer, row).start()
        part_in[d, row] = part[slot, pl.ds(pl.multiple_of(row * slab, slab), slab)]

        @pl.when(d + 2 < days)
        def _():
            get_load(d + 2).start()

    def exposures(d):
        for peer in row_peers():
            part_copy(d, row, peer).wait_recv()
        total = part_in[d, 0]
        for r in range(1, rows):
            total = total + part_in[d, r]
        own_spec[d] = total[:, factors:]
        exp_rows[d, pl.ds(pl.multiple_of(row * slab, slab), slab)] = total[:, :factors]
        exp_cols[d, col] = total[:, :factors]
        for peer in col_peers():
            exp_col_copy(d, peer, col).start()
        for peer in row_peers():
            exp_row_copy(d, peer, row).start()

    def products(d):
        slot = d % 2
        get_fcov(d).wait()
        for peer in col_peers():
            exp_col_copy(d, col, peer).wait_recv()
        left = jnp.zeros((slab, factors), F32)
        for j in range(cols):
            left = left + by_dim(
                exp_cols[d, j], fcov[slot, :, pl.ds(j * factors, factors)], 1, HIGHEST
            )

        @pl.when(d + 2 < days)
        def _():
            get_fcov(d + 2).start()

        for peer in row_peers():
            exp_row_copy(d, row, peer).wait_recv()
        for j in range(cols):
            prod[d, j] = by_dim(left, exp_rows[d, pl.ds(j * ports, ports)], 1, HIGHEST)
        for peer in col_peers():
            prod_copy(d, peer, col).start()
        prod_in[d, col] = prod[d, col]

    def finish(d):
        for peer in col_peers():
            prod_copy(d, col, peer).wait_recv()
        total = own_spec[d]
        for j in range(cols):
            total = total + prod_in[d, j]
        out_ref[d] = total

    for d in range(days):
        own_weights(d).start()
    for d in range(min(2, days)):
        get_load(d).start()
        get_fcov(d).start()

    barrier = pltpu.get_barrier_semaphore()
    for peer in row_peers():
        pl.semaphore_signal(
            barrier, inc=1, device_id=to_row(peer), device_id_type=pl.DeviceIdType.MESH
        )
    for peer in col_peers():
        pl.semaphore_signal(
            barrier, inc=1, device_id=to_col(peer), device_id_type=pl.DeviceIdType.MESH
        )
    pl.semaphore_wait(barrier, rows + cols - 2)

    send_own(0)
    if days > 1:
        send_own(1)

    def turn(t, carry):
        def stage(lag, what):
            @pl.when((t >= lag) & (t - lag < days))
            def _():
                what(t - lag)

        @pl.when(t + 2 < days)
        def _():
            send_own(t + 2)

        stage(0, pass_on)
        stage(2, exposures)
        stage(3, products)
        stage(4, finish)
        stage(1, partial_sums)
        return carry

    lax.fori_loop(0, days + 4, turn, 0)

    def drain(d, carry):
        gather(d, 0, col).wait_send()
        gather(d, 1, col).wait_send()
        gather(d, 2, near_x).wait_send()
        gather(d, 3, near_y).wait_send()
        for peer in row_peers():
            exp_row_copy(d, peer, row).wait_send()
        for peer in col_peers():
            exp_col_copy(d, peer, col).wait_send()
            prod_copy(d, peer, col).wait_send()

        @pl.when(d >= days - 2)
        def _():
            for peer in row_peers():
                part_copy(d, peer, row).wait_send()

        return carry

    lax.fori_loop(0, days, drain, 0)


def fused(loadings, weights, specific, factor_cov):
    rows, cols = lax.axis_size("row"), lax.axis_size("col")
    days, assets, factors = loadings.shape
    ports = weights.shape[2]
    slab = ports * cols // rows
    scales = specific.reshape(days, assets // 128, 128)
    anywhere = pl.BlockSpec(memory_space=pl.ANY)
    inside = pl.BlockSpec(memory_space=pltpu.VMEM)
    dma = pltpu.SemaphoreType.DMA
    return pl.pallas_call(
        functools.partial(kernel, rows, cols),
        out_shape=jax.ShapeDtypeStruct((days, slab, ports), F32),
        in_specs=[anywhere, anywhere, inside, anywhere],
        out_specs=inside,
        scratch_shapes=[
            pltpu.VMEM((days, cols, assets, ports), BF16),
            pltpu.VMEM((2, assets, factors), BF16),
            pltpu.VMEM((2, factors, cols * factors), F32),
            pltpu.VMEM((assets, ports), BF16),
            pltpu.VMEM((2, cols * ports, factors + ports), F32),
            pltpu.VMEM((days, rows, slab, factors + ports), F32),
            pltpu.VMEM((days, cols * ports, factors), F32),
            pltpu.VMEM((days, cols, slab, factors), F32),
            pltpu.VMEM((days, slab, ports), F32),
            pltpu.VMEM((days, cols, slab, ports), F32),
            pltpu.VMEM((days, cols, slab, ports), F32),
            dma((days,)), dma((2,)), dma((2,)),
            dma((days, 4)), dma((days, 4)),
            dma((days, rows)), dma((days, rows)),
            dma((days, rows)), dma((days, rows)),
            dma((days, cols)), dma((days, cols)),
            dma((days, cols)), dma((days, cols)),
        ],
        compiler_params=pltpu.CompilerParams(
            collective_id=0, has_side_effects=True, vmem_limit_bytes=67_000_000
        ),
        name="covariance",
    )(loadings, weights, scales, factor_cov)


def plain(loadings, weights, specific, factor_cov):
    factor_cols = loadings.shape[2]
    port_cols = weights.shape[2]
    total_ports = port_cols * lax.axis_size("col")
    port_rows = total_ports // lax.axis_size("row")
    row_start = lax.axis_index("row") * port_rows
    weighted = (specific[:, :, None] * weights.astype(F32)).astype(BF16)
    fragment = lax.all_gather(weights, "col", axis=2, tiled=True)
    exposure_part = jnp.einsum("dar,dap->drp", loadings, fragment, preferred_element_type=F32)
    specific_term = jnp.einsum("dak,dap->dkp", weighted, fragment, preferred_element_type=F32)
    joined = jnp.concatenate([exposure_part, specific_term], axis=1)
    exposure = lax.psum(joined[:, :factor_cols, :], "row")
    specific_block = lax.psum_scatter(
        joined[:, factor_cols:, :], "row", scatter_dimension=2, tiled=True
    )
    exposure_rows = lax.dynamic_slice_in_dim(exposure, row_start, port_rows, 2)
    left_part = jnp.einsum("dri,drs->dis", exposure_rows, factor_cov, precision=HIGHEST)
    left = lax.psum(left_part, "col")
    exposure_cols = lax.all_to_all(exposure, "col", split_axis=2, concat_axis=1, tiled=True)
    factor_block = jnp.einsum("dir,drk->dik", left, exposure_cols, precision=HIGHEST)
    return factor_block + jnp.swapaxes(specific_block, 1, 2)


def solution(mesh):
    in_specs = (P(None, "row", "col"), P(None, "row", "col"), P(None, "row"), P(None, "col", None))
    out_specs = P(None, "row", "col")
    body = fused if mesh.shape["col"] == 4 else plain
    return jax.shard_map(body, mesh=mesh, in_specs=in_specs, out_specs=out_specs, check_vma=False)
```

```python
import functools

import jax
import jax.numpy as jnp
from jax import lax
from jax.experimental import pallas as pl
from jax.experimental.pallas import tpu as pltpu
from jax.sharding import PartitionSpec as P

F32, BF16 = jnp.float32, jnp.bfloat16
HIGHEST = lax.Precision.HIGHEST
CUTS, AHEAD = 4, 2
LAGS = (4, 5, 7, 9, 12, 15)


def by_dim(a, b, dim, precision=None):
    return lax.dot_general(
        a, b, (((dim,), (dim,)), ((), ())), precision=precision, preferred_element_type=F32
    )


def kernel(
    rows, cols, cuts, load_hbm, weight_hbm, spec_ref, fcov_hbm, out_ref,
    held, load, fcov, weighted, part, mate_in, pair, part_in, exp_rows, exp_cols, own_spec, prod, prod_in,
    w_sem, l_sem, f_sem, g_send, g_recv, m_send, m_recv, p_send, p_recv,
    er_send, er_recv, ec_send, ec_recv, q_send, q_recv,
):
    days, assets, factors = load_hbm.shape
    ports = weight_hbm.shape[2]
    slab = ports * cols // rows
    row, col = lax.axis_index("row"), lax.axis_index("col")
    near_x = col + 1 - 2 * (col % 2)
    near_y = (col + 2) % 4
    far = 3 - col
    chips, per = rows // 2, rows // cols
    piece = assets // cuts
    mine, core = row // 2, row % 2
    mate = row + 1 - 2 * core

    def to_row(r):
        return {"row": r, "col": col}

    def to_col(c):
        return {"row": row, "col": c}

    def remote(src, dst, send, recv, where):
        return pltpu.make_async_remote_copy(
            src_ref=src, dst_ref=dst, send_sem=send, recv_sem=recv,
            device_id=where, device_id_type=pl.DeviceIdType.MESH,
        )

    def lanes(buf, send, recv, d, u, start, size, lane, block):
        half = size // 2
        if lane == 2:
            size = half
        if lane == 3:
            start, size = start + half, half
        ref = buf.at[d, block, pl.ds(start, size)]
        where = near_x if lane in (0, 3) else near_y
        return remote(ref, ref, send.at[u, lane], recv.at[u, lane], to_col(where))

    def gather(u, lane, block):
        start = pl.multiple_of((u % cuts) * piece, piece)
        return lanes(held, g_send, g_recv, u // cuts, u, start, piece, lane, block)

    def exp_gather(d, lane, block):
        return lanes(exp_cols, ec_send, ec_recv, d, d, 0, slab, lane, block)

    def own_weights(d):
        return pltpu.make_async_copy(weight_hbm.at[d], held.at[d, col], w_sem.at[d])

    def get_load(d):
        return pltpu.make_async_copy(load_hbm.at[d], load.at[d % 2], l_sem.at[d % 2])

    def get_fcov(d):
        return pltpu.make_async_copy(fcov_hbm.at[d], fcov.at[d % 2], f_sem.at[d % 2])

    def mate_copy(d):
        return remote(
            part.at[d % 2, 1 - core], mate_in.at[d], m_send.at[d], m_recv.at[d], to_row(mate)
        )

    def part_copy(d, other, landed):
        return remote(
            pair.at[d % 2, other], part_in.at[d, landed],
            p_send.at[d, other], p_recv.at[d, landed], to_row(2 * other + core),
        )

    def exp_row_copy(d, slot, landed, other):
        ref = exp_rows.at[d, pl.ds(pl.multiple_of(landed * slab, slab), slab)]
        return remote(ref, ref, er_send.at[d, slot], er_recv.at[d, landed], to_row(other))

    def prod_copy(d, other, landed):
        return remote(
            prod.at[d, other], prod_in.at[d, landed],
            q_send.at[d, other], q_recv.at[d, landed], to_col(other),
        )

    def row_peers():
        return [(row + step) % rows for step in range(1, rows)]

    def chip_peers():
        return [(mine + step) % chips for step in range(1, chips)]

    def col_peers():
        return [near_x, near_y, far]

    def send_own(u):
        @pl.when(u % cuts == 0)
        def _():
            own_weights(u // cuts).wait()

        gather(u, 0, col).start()
        gather(u, 1, col).start()

    def pass_on(u):
        gather(u, 0, near_x).wait_recv()
        gather(u, 2, near_x).start()
        gather(u, 1, near_y).wait_recv()
        gather(u, 3, near_y).start()

    def sum_block(d, j):
        slot = d % 2
        lhs = held[d, j]
        by_factor = by_dim(lhs, load[slot], 0)
        by_port = by_dim(lhs, weighted[...], 0)
        for i in range(per):
            span = slice(i * slab, (i + 1) * slab)
            place = j * (per // 2) + i // 2
            part[slot, i % 2, place, :, pl.ds(0, factors)] = by_factor[span]
            part[slot, i % 2, place, :, pl.ds(factors, ports)] = by_port[span]

    def near_sums(d):
        scales = spec_ref[d]
        groups = scales.shape[0]
        copies = -(-128 // groups)
        tall = jnp.concatenate([scales] * copies, axis=0).T
        for i in range(groups):
            span = pl.ds(i * 128, 128)
            block = held[d, col, span].astype(F32) * tall[:, i : i + 1]
            weighted[span] = block.astype(BF16)

        @pl.when(d >= 2)
        def _():
            mate_copy(d - 2).wait_send()
            for peer in chip_peers():
                part_copy(d - 2, peer, mine).wait_send()

        get_load(d).wait()

        def near_block(i, carry):
            sum_block(d, (far + 1 + i) % cols)
            return carry

        lax.fori_loop(0, cols - 1, near_block, 0)

    def far_sums(d):
        slot = d % 2
        for q in range(cuts):
            gather(d * cuts + q, 2, far).wait_recv()
            gather(d * cuts + q, 3, far).wait_recv()
        sum_block(d, far)
        mate_copy(d).start()

        @pl.when(d + 2 < days)
        def _():
            get_load(d + 2).start()

        mate_copy(d).wait_recv()
        for peer in chip_peers():
            pair[slot, peer] = part[slot, core, peer] + mate_in[d, peer]
            part_copy(d, peer, mine).start()
        part_in[d, mine] = part[slot, core, mine] + mate_in[d, mine]

    def exposures(d):
        for peer in chip_peers():
            part_copy(d, mine, peer).wait_recv()
        total = part_in[d, 0]
        for z in range(1, chips):
            total = total + part_in[d, z]
        own_spec[d] = total[:, factors:]
        exp_rows[d, pl.ds(pl.multiple_of(row * slab, slab), slab)] = total[:, :factors]
        exp_cols[d, col] = total[:, :factors]
        exp_gather(d, 0, col).start()
        exp_gather(d, 1, col).start()
        for peer in chip_peers():
            exp_row_copy(d, 2 * peer + core, row, 2 * peer + core).start()
        exp_row_copy(d, mate, row, mate).start()

    def share(d):
        exp_gather(d, 0, near_x).wait_recv()
        exp_gather(d, 2, near_x).start()
        exp_gather(d, 1, near_y).wait_recv()
        exp_gather(d, 3, near_y).start()
        for peer in chip_peers():
            exp_row_copy(d, row, 2 * peer + core, mate).wait_recv()
            exp_row_copy(d, 2 * peer + 1 - core, 2 * peer + core, mate).start()

    def products(d):
        slot = d % 2
        get_fcov(d).wait()
        exp_gather(d, 2, far).wait_recv()
        exp_gather(d, 3, far).wait_recv()
        left = jnp.zeros((slab, factors), F32)
        for j in range(cols):
            left = left + by_dim(
                exp_cols[d, j], fcov[slot, :, pl.ds(j * factors, factors)], 1, HIGHEST
            )

        @pl.when(d + 2 < days)
        def _():
            get_fcov(d + 2).start()

        exp_row_copy(d, row, mate, mate).wait_recv()
        for peer in chip_peers():
            exp_row_copy(d, row, 2 * peer + 1 - core, mate).wait_recv()
        for j in range(cols):
            prod[d, j] = by_dim(left, exp_rows[d, pl.ds(j * ports, ports)], 1, HIGHEST)
        for peer in col_peers():
            prod_copy(d, peer, col).start()
        prod_in[d, col] = prod[d, col]

    def finish(d):
        for peer in col_peers():
            prod_copy(d, col, peer).wait_recv()
        total = own_spec[d]
        for j in range(cols):
            total = total + prod_in[d, j]
        out_ref[d] = total

    for d in range(days):
        own_weights(d).start()
    for d in range(min(2, days)):
        get_load(d).start()
        get_fcov(d).start()

    barrier = pltpu.get_barrier_semaphore()
    for peer in row_peers():
        pl.semaphore_signal(
            barrier, inc=1, device_id=to_row(peer), device_id_type=pl.DeviceIdType.MESH
        )
    for peer in col_peers():
        pl.semaphore_signal(
            barrier, inc=1, device_id=to_col(peer), device_id_type=pl.DeviceIdType.MESH
        )
    pl.semaphore_wait(barrier, rows + cols - 2)

    for u in range(AHEAD):
        send_own(u)

    def turn(t, carry):
        def stage(lag, what):
            @pl.when((t >= lag) & ((t - lag) % cuts == 0) & (t - lag < cuts * days))
            def _():
                what((t - lag) // cuts)

        @pl.when(t + AHEAD < cuts * days)
        def _():
            send_own(t + AHEAD)

        @pl.when(t < cuts * days)
        def _():
            pass_on(t)

        for lag, what in zip(LAGS, (near_sums, far_sums, exposures, share, products, finish)):
            stage(lag, what)
        return carry

    lax.fori_loop(0, cuts * (days - 1) + LAGS[-1] + 1, turn, 0)

    def drain(d, carry):
        for u in range(cuts):
            gather(d * cuts + u, 0, col).wait_send()
            gather(d * cuts + u, 1, col).wait_send()
            gather(d * cuts + u, 2, near_x).wait_send()
            gather(d * cuts + u, 3, near_y).wait_send()
        exp_gather(d, 0, col).wait_send()
        exp_gather(d, 1, col).wait_send()
        exp_gather(d, 2, near_x).wait_send()
        exp_gather(d, 3, near_y).wait_send()
        exp_row_copy(d, mate, row, mate).wait_send()
        for peer in chip_peers():
            exp_row_copy(d, 2 * peer + core, row, 2 * peer + core).wait_send()
            exp_row_copy(d, 2 * peer + 1 - core, 2 * peer + core, mate).wait_send()
        for peer in col_peers():
            prod_copy(d, peer, col).wait_send()

        @pl.when(d >= days - 2)
        def _():
            mate_copy(d).wait_send()
            for peer in chip_peers():
                part_copy(d, peer, mine).wait_send()

        return carry

    lax.fori_loop(0, days, drain, 0)


def fused(loadings, weights, specific, factor_cov):
    rows, cols = lax.axis_size("row"), lax.axis_size("col")
    days, assets, factors = loadings.shape
    ports = weights.shape[2]
    slab = ports * cols // rows
    scales = specific.reshape(days, assets // 128, 128)
    anywhere = pl.BlockSpec(memory_space=pl.ANY)
    inside = pl.BlockSpec(memory_space=pltpu.VMEM)
    dma = pltpu.SemaphoreType.DMA
    return pl.pallas_call(
        functools.partial(kernel, rows, cols, CUTS),
        out_shape=jax.ShapeDtypeStruct((days, slab, ports), F32),
        in_specs=[anywhere, anywhere, inside, anywhere],
        out_specs=inside,
        scratch_shapes=[
            pltpu.VMEM((days, cols, assets, ports), BF16),
            pltpu.VMEM((2, assets, factors), BF16),
            pltpu.VMEM((2, factors, cols * factors), F32),
            pltpu.VMEM((assets, ports), BF16),
            pltpu.VMEM((2, 2, rows // 2, slab, factors + ports), F32),
            pltpu.VMEM((days, rows // 2, slab, factors + ports), F32),
            pltpu.VMEM((2, rows // 2, slab, factors + ports), F32),
            pltpu.VMEM((days, rows // 2, slab, factors + ports), F32),
            pltpu.VMEM((days, cols * ports, factors), F32),
            pltpu.VMEM((days, cols, slab, factors), F32),
            pltpu.VMEM((days, slab, ports), F32),
            pltpu.VMEM((days, cols, slab, ports), F32),
            pltpu.VMEM((days, cols, slab, ports), F32),
            dma((days,)), dma((2,)), dma((2,)),
            dma((days * CUTS, 4)), dma((days * CUTS, 4)),
            dma((days,)), dma((days,)),
            dma((days, rows // 2)), dma((days, rows // 2)),
            dma((days, rows)), dma((days, rows)),
            dma((days, cols)), dma((days, cols)),
            dma((days, cols)), dma((days, cols)),
        ],
        compiler_params=pltpu.CompilerParams(
            collective_id=0, has_side_effects=True, vmem_limit_bytes=67_000_000
        ),
        name="covariance",
    )(loadings, weights, scales, factor_cov)


def plain(loadings, weights, specific, factor_cov):
    factor_cols = loadings.shape[2]
    port_cols = weights.shape[2]
    total_ports = port_cols * lax.axis_size("col")
    port_rows = total_ports // lax.axis_size("row")
    row_start = lax.axis_index("row") * port_rows
    weighted = (specific[:, :, None] * weights.astype(F32)).astype(BF16)
    fragment = lax.all_gather(weights, "col", axis=2, tiled=True)
    exposure_part = jnp.einsum("dar,dap->drp", loadings, fragment, preferred_element_type=F32)
    specific_term = jnp.einsum("dak,dap->dkp", weighted, fragment, preferred_element_type=F32)
    joined = jnp.concatenate([exposure_part, specific_term], axis=1)
    exposure = lax.psum(joined[:, :factor_cols, :], "row")
    specific_block = lax.psum_scatter(
        joined[:, factor_cols:, :], "row", scatter_dimension=2, tiled=True
    )
    exposure_rows = lax.dynamic_slice_in_dim(exposure, row_start, port_rows, 2)
    left_part = jnp.einsum("dri,drs->dis", exposure_rows, factor_cov, precision=HIGHEST)
    left = lax.psum(left_part, "col")
    exposure_cols = lax.all_to_all(exposure, "col", split_axis=2, concat_axis=1, tiled=True)
    factor_block = jnp.einsum("dir,drk->dik", left, exposure_cols, precision=HIGHEST)
    return factor_block + jnp.swapaxes(specific_block, 1, 2)


def solution(mesh):
    in_specs = (P(None, "row", "col"), P(None, "row", "col"), P(None, "row"), P(None, "col", None))
    out_specs = P(None, "row", "col")
    rows, cols = mesh.shape["row"], mesh.shape["col"]
    body = fused if cols == 4 and rows % (2 * cols) == 0 else plain
    return jax.shard_map(body, mesh=mesh, in_specs=in_specs, out_specs=out_specs, check_vma=False)
```
